32 devices in a mesh: dp: 2 (over x), tensor: 4 (over y, core), grid: 4 (over z).
Axes of the slice: x: 2, y: 2, z: 4, core: 2. Of those that a mesh axis runs over, the one named last changes fastest.
Arguments:
- tokens: bfloat16 [1536, 8192], P('dp', 'grid'), may hold values from -6 to 6
- cotangents: bfloat16 [2, 1536, 1024], P(None, 'dp', 'tensor'), may hold values from -0.03125 to 0.03125
- left_stat: float32 [2, 8192, 8192], P(None, ('dp', 'tensor'), 'grid'), may hold values from -6 to 6
- right_stat: float32 [2, 1024, 1024], P(None, ('dp', 'tensor'), 'grid'), may hold values from -6 to 6
- left_root: bfloat16 [2, 8192, 8192], P(None, ('dp', 'tensor'), 'grid'), may hold values from -0.3125 to 0.3125
- right_root: bfloat16 [2, 1024, 1024], P(None, 'grid'), as said below
- momentum: float32 [2, 8192, 1024], P(None, ('dp', 'tensor', 'grid')), may hold values from -6 to 6
Outputs:
- new_left: float32 [2, 8192, 8192], P(None, ('dp', 'tensor'), 'grid')
- new_right: float32 [2, 1024, 1024], P(None, ('dp', 'tensor'), 'grid')
- new_momentum: float32 [2, 8192, 1024], P(None, ('dp', 'tensor', 'grid'))
The draws below stay inside these ranges and needn't reach their ends.
Inputs may be any that keep to these rules, and one draw needn't show every extreme that they name: `right_root`: each of the two factors is exactly symmetric.
All inputs are finite; a program needn't handle non-finite values.
Results may differ from the reference program's by a relative error of at most 0.0023.
Values may be sent and summed in bfloat16 or wider, within the bound.
No kernel may reach another device: no remote copies, remote signals or barrier semaphores. Data moves between devices by JAX's collectives and lax.ppermute only.
A program may use at most 128 MiB of HBM per device.

```python
import math
import jax
import jax.numpy as jnp
from jax import lax

D = 8192
KV = 1024
TOKENS = 1536


def draw_right_root(key, part):
    raw = jax.random.normal(key, (2, KV, KV), jnp.float32)
    symmetric = (raw + jnp.swapaxes(raw, 1, 2)) * (0.35 / math.sqrt(KV))
    return (symmetric + jnp.eye(KV, dtype=jnp.float32)).astype(jnp.bfloat16)


def block_scale(stream_key, extent, cuts, low, high):
    factor_of, own = 1.0, jax.random.fold_in(stream_key, 6)
    for position, blocks in cuts:
        heights = jnp.exp(jax.random.uniform(jax.random.fold_in(own, position), (blocks,), jnp.float32, low / len(cuts), high / len(cuts)))
        factor_of = factor_of * jnp.repeat(heights, extent[position] // blocks).reshape([-1 if axis == position else 1 for axis in range(len(extent))])
    return factor_of


def noise(key, extent, scale, most, cuts=(), held_as=jnp.bfloat16):
    drawn = scale * jax.random.normal(key, extent, jnp.float32)
    if cuts:
        drawn = drawn * block_scale(key, extent, cuts, -0.22, 0.18)
    return jnp.clip(drawn, -most, most).astype(held_as)


def setup_inputs(seed: int = 0) -> dict:
    arg_keys = jax.random.split(jax.random.key(seed), 8)
    return {
        "tokens": noise(arg_keys[0], (TOKENS, D), 1.0, 6.0, ((0, 2), (1, 4))),
        "cotangents": noise(arg_keys[1], (2, TOKENS, KV), (25 * TOKENS) ** -0.5, 0.03125, ((1, 2), (2, 4))),
        "left_stat": noise(arg_keys[2], (2, D, D), 1.0, 6.0, ((1, 8), (2, 4)), jnp.float32),
        "right_stat": noise(arg_keys[3], (2, KV, KV), 1.0, 6.0, ((1, 8), (2, 4)), jnp.float32),
        "left_root": noise(arg_keys[4], (2, D, D), (D // 25) ** -0.5, 0.3125, ((1, 8), (2, 4))),
        "right_root": draw_right_root(jax.random.fold_in(arg_keys[7], 71), 0),
        "momentum": noise(arg_keys[6], (2, D, KV), 1.0, 6.0, ((1, 32),), jnp.float32),
    }


stat_decay = 0.9
momentum_decay = 0.9


def reference(tokens, cotangents, left_stat, right_stat, left_root, right_root, momentum):
    left_list = []
    right_list = []
    moment_list = []
    for project in range(2):
        gradient = jnp.dot(tokens.T, cotangents[project], preferred_element_type=jnp.float32)
        rounded = gradient.astype(jnp.bfloat16)
        gram_left = jnp.dot(rounded, rounded.T, preferred_element_type=jnp.float32)
        gram_right = jnp.dot(rounded.T, rounded, preferred_element_type=jnp.float32)
        left_list.append(stat_decay * left_stat[project] + (1.0 - stat_decay) * gram_left)
        right_list.append(stat_decay * right_stat[project] + (1.0 - stat_decay) * gram_right)
        applied = jnp.dot(left_root[project], rounded, preferred_element_type=jnp.float32)
        factor = right_root[project].astype(jnp.float32)
        update = jnp.dot(applied, factor, precision=lax.Precision.HIGHEST, preferred_element_type=jnp.float32)
        moment_list.append(momentum_decay * momentum[project] + update)
    return jnp.stack(left_list), jnp.stack(right_list), jnp.stack(moment_list)
```

```python
import jax
import jax.numpy as jnp
from jax import lax
from jax.sharding import PartitionSpec as P

stat_decay = 0.9
momentum_decay = 0.9
bf16, f32 = jnp.bfloat16, jnp.float32


def xor_send(x, axis, k):
    n = lax.axis_size(axis)
    return lax.ppermute(x, axis, [(i, i ^ k) for i in range(n)])


def bit_of(axis, k):
    return (lax.axis_index(axis) // k) % 2


def pair(own, got, bit):
    first = bit == 0
    return jnp.stack([jnp.where(first, own, got), jnp.where(first, got, own)])


def bits_down(n):
    out = []
    k = n // 2
    while k:
        out.append(k)
        k //= 2
    return out


def part(x, bit, axis):
    return lax.dynamic_index_in_dim(x, bit, axis, keepdims=False)


def gather_tokens(tokens):
    n = lax.axis_size("dp")
    rows = tokens.shape[0]
    core = bit_of("tensor", 1)
    half = lax.dynamic_slice_in_dim(tokens, core * (rows // 2), rows // 2, 0)
    out = [tokens]
    for k in range(1, n):
        got = xor_send(half, "dp", k)
        other = xor_send(got, "tensor", 1)
        out.append(pair(got, other, core).reshape(rows, -1))
    return jnp.concatenate(out, 0)


def gather_cotangents(cot):
    n, m = lax.axis_size("dp"), lax.axis_size("tensor")
    x = jnp.concatenate([cot] + [xor_send(cot, "dp", k) for k in range(1, n)], 0)
    x = x[None]
    for k in bits_down(m):
        got = xor_send(x, "tensor", k)
        both = pair(x, got, bit_of("tensor", k))
        x = jnp.swapaxes(both, 0, 1).reshape(-1, *x.shape[1:])
    return jnp.swapaxes(x, 0, 1).reshape(x.shape[1], -1)


def row_tokens(tokens, block_rows):
    n, m, g = lax.axis_size("dp"), lax.axis_size("tensor"), lax.axis_size("grid")
    per = tokens.shape[1] // block_rows
    d, t, z = lax.axis_index("dp"), lax.axis_index("tensor"), lax.axis_index("grid")

    def source(dd, tt):
        return (dd * m + tt) // per

    offset = ((d * m + t) % per) * block_rows if m % per else (t % per) * block_rows
    own = lax.dynamic_slice_in_dim(tokens, offset, block_rows, 1)
    sources = [{source(dd, tt) for dd in range(n)} for tt in range(m)]
    arrived = {0: own}
    for sign in (1, -1):
        held = own
        for step in range(1, g):
            pairs = []
            for tt in range(m):
                for zz in range(g):
                    start = zz - sign * (step - 1)
                    if start in sources[tt] and 0 <= zz + sign < g:
                        pairs.append((tt * g + zz, tt * g + zz + sign))
            if not pairs:
                break
            held = lax.ppermute(held, ("tensor", "grid"), pairs)
            arrived[-sign * step] = held

    def block(dd):
        offsets = sorted({source(e, tt) - zz for e in range(n) for tt in range(m) for zz in range(g)} & set(arrived))
        want = source(dd, t) - z
        out = arrived[offsets[0]]
        for o in offsets[1:]:
            out = jnp.where(want == o, arrived[o], out)
        return out

    out = [block(d)]
    for k in range(1, n):
        out.append(xor_send(block(d ^ k), "dp", k))
    return jnp.concatenate(out, 0)


def gather_right_root(right_root):
    m = lax.axis_size("tensor")
    rows = right_root.shape[1] // m
    x = lax.dynamic_slice_in_dim(right_root, lax.axis_index("tensor") * rows, rows, 1)
    x = jnp.swapaxes(x, 0, 1)[None]
    for k in bits_down(lax.axis_size("grid"))[::-1]:
        got = xor_send(x, "grid", k)
        x = pair(x, got, bit_of("grid", k)).reshape(-1, *x.shape[1:])
    x = x[None]
    for k in bits_down(m)[::-1]:
        got = xor_send(x, "tensor", k)
        x = pair(x, got, bit_of("tensor", k)).reshape(-1, *x.shape[1:])
    return jnp.transpose(x, (3, 1, 0, 2, 4)).reshape(right_root.shape[0], -1, right_root.shape[2])


def dot(a, b, dims):
    return lax.dot_general(a, b, (dims, ((), ())), preferred_element_type=f32)


def scatter_applied(left_root, grad):
    g = lax.axis_size("grid")
    rows = left_root.shape[0] // g
    steps = bits_down(g)[::-1]
    lhs = left_root.reshape(g // 2, 2, rows, left_root.shape[1])
    bit = bit_of("grid", 1)

    def product(which):
        x = part(lhs, which, 1).reshape(-1, left_root.shape[1])
        return dot(x, grad, ((1,), (0,)))

    got = xor_send(product(1 - bit).astype(bf16), "grid", 1)
    total = (product(bit) + got.astype(f32)).reshape(g // 2, rows, -1)
    for k in steps[1:]:
        bit = bit_of("grid", k)
        total = total.reshape(-1, 2, rows, total.shape[-1])
        got = xor_send(part(total, 1 - bit, 1).astype(bf16), "grid", k)
        total = part(total, bit, 1) + got.astype(f32)
    return total.reshape(rows, -1)


def scatter_right(term, learners):
    n, m = lax.axis_size("dp"), lax.axis_size("tensor")
    p, rows, cols = term.shape
    order = [("tensor", 1)] + [("dp", k) for k in bits_down(n)] + [("tensor", k) for k in bits_down(m)[:-1]]
    sizes = {("dp", k): 0 for k in bits_down(n)}
    names = [("dp", k) for k in bits_down(n)] + [("tensor", k) for k in bits_down(m)]
    x = term.reshape(p, *([2] * len(names)), rows // (n * m), cols)
    left = list(names)
    for i, (axis, k) in enumerate(order):
        at = 1 + left.index((axis, k))
        left.remove((axis, k))
        bit = bit_of(axis, k)
        send = part(x, 1 - bit, at)
        if i == 0:
            got = xor_send(send, axis, k)
        else:
            got = xor_send(send.astype(bf16), axis, k).astype(f32)
        x = part(x, bit, at) + got
    return x


def move_inputs(tokens, cotangents, left_stat, right_stat, left_root, right_root, momentum):
    projections = cotangents.shape[0]
    block_rows = left_stat.shape[1]
    all_tokens = gather_tokens(tokens)
    cots = [gather_cotangents(cotangents[p]) for p in range(projections)]
    root = gather_right_root(right_root)
    rows_tokens = row_tokens(tokens, block_rows)

    new_momentum, new_left, right_terms = [], [], []
    width = right_stat.shape[2]
    for p in range(projections):
        grad = dot(all_tokens, cots[p], ((0,), (0,))).astype(bf16)
        applied = scatter_applied(left_root[p], grad)
        high = lax.reduce_precision(applied, 8, 7)
        low = (applied - high).astype(bf16)
        update = dot(high.astype(bf16), root[p], ((1,), (0,))) + dot(low, root[p], ((1,), (0,)))
        new_momentum.append(momentum_decay * momentum[p] + update)
        own = dot(rows_tokens, cots[p], ((0,), (0,))).astype(bf16)
        gram = dot(own, grad, ((1,), (1,)))
        new_left.append(stat_decay * left_stat[p] + (1.0 - stat_decay) * gram)
        columns = lax.dynamic_slice_in_dim(own, lax.axis_index("grid") * width, width, 1)
        right_terms.append(dot(own, columns, ((0,), (0,))))
    right = scatter_right(jnp.stack(right_terms), None)
    new_right = stat_decay * right_stat + (1.0 - stat_decay) * right
    return jnp.stack(new_left), new_right, jnp.stack(new_momentum)


def spread(shard, axis, root):
    mine = lax.axis_index(axis) == root
    return lax.psum(jnp.where(mine, shard, jnp.zeros_like(shard)), axis)


def move_gradients(tokens, cotangents, left_stat, right_stat, left_root, right_root, momentum):
    partial_grad = jnp.einsum("tr,pto->pro", tokens, cotangents, preferred_element_type=jnp.float32)
    summed = lax.psum(partial_grad, "dp")
    grad_rows = lax.all_gather(summed.astype(jnp.bfloat16), "tensor", axis=2, tiled=True)
    block_rows = left_stat.shape[1]
    grid_rows = left_stat.shape[2]
    learner = lax.axis_index("dp") * lax.axis_size("tensor") + lax.axis_index("tensor")
    first_row = learner * block_rows
    source = first_row // grid_rows
    offset = first_row % grid_rows
    selected = lax.dynamic_slice_in_dim(grad_rows, offset, block_rows, 1)
    own_rows = spread(selected, "grid", source)
    gram_left = jnp.einsum("pak,pbk->pab", own_rows, grad_rows, preferred_element_type=jnp.float32)
    new_left = stat_decay * left_stat + (1.0 - stat_decay) * gram_left
    column_width = right_stat.shape[2]
    column_block = lax.dynamic_slice_in_dim(
        own_rows, lax.axis_index("grid") * column_width, column_width, 2
    )
    right_term = jnp.einsum(
        "pak,pac->pkc", own_rows, column_block, preferred_element_type=jnp.float32
    )
    gram_right = lax.psum_scatter(right_term, ("dp", "tensor"), scatter_dimension=1, tiled=True)
    new_right = stat_decay * right_stat + (1.0 - stat_decay) * gram_right
    applied = lax.psum_scatter(
        jnp.einsum("pab,pbk->apk", left_root, grad_rows, preferred_element_type=jnp.float32),
        "grid",
        scatter_dimension=0,
        tiled=True,
    )
    widened_rows = lax.all_gather(right_root, "grid", axis=1, tiled=True).astype(jnp.float32)
    update = jnp.einsum(
        "mpk,pkc->mpc",
        applied,
        widened_rows,
        precision=lax.Precision.HIGHEST,
        preferred_element_type=jnp.float32,
    )
    new_momentum = momentum_decay * momentum + jnp.transpose(update, (1, 0, 2))
    return (new_left, new_right, new_momentum)


def shards(tokens, cotangents, left_stat, right_stat, left_root, right_root, momentum):
    args = (tokens, cotangents, left_stat, right_stat, left_root, right_root, momentum)
    n, m = lax.axis_size("dp"), lax.axis_size("tensor")
    inputs = tokens.size * (n - 1) + cotangents.size * (n * m - 1)
    gradients = cotangents.shape[0] * tokens.shape[1] * cotangents.shape[2] * (2 * (n - 1) + m - 1)
    return move_inputs(*args) if inputs < gradients else move_gradients(*args)


def solution(mesh):
    return jax.shard_map(
        shards,
        mesh=mesh,
        in_specs=(
            P("dp", "grid"),
            P(None, "dp", "tensor"),
            P(None, ("dp", "tensor"), "grid"),
            P(None, ("dp", "tensor"), "grid"),
            P(None, ("dp", "tensor"), "grid"),
            P(None, "grid", None),
            P(None, ("dp", "tensor", "grid"), None),
        ),
        out_specs=(
            P(None, ("dp", "tensor"), "grid"),
            P(None, ("dp", "tensor"), "grid"),
            P(None, ("dp", "tensor", "grid"), None),
        ),
        check_vma=False,
    )
```
